512 devices in a mesh: seq: 128 (over y, z, core), head: 4 (over x).
Axes of the slice: x: 4, y: 8, z: 8, core: 2. Of those that a mesh axis runs over, the one named last changes fastest.
Arguments:
- queries: bfloat16 [32768, 4096], P('seq', 'head'), may hold values from -6 to 6
- keys: bfloat16 [32768, 1024], P('seq', 'head'), may hold values from -6 to 6
- values: bfloat16 [32768, 1024], P('seq', 'head'), may hold values from -15 to 15
- selected: int32 [512, 8, 16], P('seq', 'head'), may hold values from -1 to 511, as said below
- norm_gain: bfloat16 [4096], P('head'), may hold values from 0.099609375 to 1.8984375
Outputs:
- normalized: bfloat16 [32768, 4096], P('seq', 'head')
The draws below stay inside these ranges and needn't reach their ends.
Inputs may be any that keep to these rules, and one draw needn't show every extreme that they name: selected[b, g] lists b first, then 0 (or -1 where b = 0), then distinct blocks above 0 and below b, or -1. Over the query blocks of one index of seq and the KV heads of one index of head, the blocks named that belong to another index of seq form at most 2 distinct (block, KV head) pairs per such index.
All inputs are finite; a program needn't handle non-finite values.
Results may differ from the reference program's by a relative error of at most 0.0047.
Values may be sent and summed in bfloat16 or wider, within the bound.
No kernel may reach another device: no remote copies, remote signals or barrier semaphores. Data moves between devices by JAX's collectives and lax.ppermute only.
A program may use at most 64 MiB of HBM per device.

```python
import math
import jax
import jax.numpy as jnp
from jax import lax

QHEADS = 32
KVHEADS = 8
HEAD_DIM = 128
BLOCK = 64
TOPK = 16
TOK_DEV = 256
TOKENS = 32768


def draw_keys(key, part):
    base = jnp.clip(jax.random.normal(jax.random.fold_in(key, 11), (TOKENS, KVHEADS * HEAD_DIM), jnp.float32), -5.0, 5.0)
    return base.astype(jnp.bfloat16)


def draw_queries(key, part):
    base = jnp.clip(jax.random.normal(jax.random.fold_in(key, 17), (TOKENS, QHEADS * HEAD_DIM), jnp.float32), -5.0, 5.0)
    return base.astype(jnp.bfloat16)


def draw_values(key, part):
    base = jnp.clip(jax.random.normal(jax.random.fold_in(key, 23), (TOKENS, KVHEADS * HEAD_DIM), jnp.float32), -5.0, 5.0)
    level = (jnp.arange(KVHEADS * HEAD_DIM) // HEAD_DIM).astype(jnp.float32) / (KVHEADS - 1) - 0.5
    factor = jnp.exp(level * jnp.log(3.0))
    return (base * factor[None, :]).astype(jnp.bfloat16)


def draw_selected(key, part):
    devices = TOKENS // TOK_DEV
    per_dev = TOK_DEV // BLOCK
    tile_index_sequence = TOKENS // BLOCK
    hot = jax.random.randint(jax.random.fold_in(key, 29), (tile_index_sequence,), 0, 12) == 0
    popular_tiles = jnp.where(hot, 3000, jax.random.randint(jax.random.fold_in(key, 31), (tile_index_sequence,), 0, 600))
    offer_score = jax.random.randint(jax.random.fold_in(key, 37), (devices, KVHEADS, devices, per_dev), 0, 1000)
    offer_score = (offer_score + popular_tiles.reshape(devices, per_dev)[None, None]) * per_dev + jnp.arange(per_dev)
    unused, best = lax.top_k(offer_score, 1)
    offered = jnp.arange(per_dev)[None, None, None, :] == best
    offered = offered.reshape(devices, KVHEADS, tile_index_sequence)
    prospective_tile = jnp.arange(tile_index_sequence, dtype=jnp.int32)
    owner = prospective_tile // per_dev
    noise_key = jax.random.fold_in(key, 41)

    def one_block(number):
        reader = number // per_dev
        allowed = lax.dynamic_index_in_dim(offered, reader, axis=0, keepdims=False)
        distant_tile_approved = (owner != 0)[None, :] & allowed
        assigned = distant_tile_approved & (owner % per_dev == number % per_dev)[None, :]
        admissible_indicator = (prospective_tile >= 1)[None, :] & (prospective_tile < number)[None, :] & ((owner == reader)[None, :] | distant_tile_approved)
        relevance_perturbation = jax.random.randint(jax.random.fold_in(noise_key, number), (KVHEADS, tile_index_sequence), 0, 1000)
        relevance_increment = jnp.where(assigned, 20000, jnp.where(distant_tile_approved, 5000, 0))
        tile_relevance = jnp.where(admissible_indicator, (relevance_perturbation + popular_tiles[None, :] + relevance_increment) * tile_index_sequence + prospective_tile[None, :], -1 - prospective_tile[None, :])
        top_val, top_idx = lax.top_k(tile_relevance, TOPK - 2)
        picks = jnp.where(top_val >= 0, top_idx, -1).astype(jnp.int32)
        own = jnp.full((KVHEADS, 1), number, jnp.int32)
        first = jnp.full((KVHEADS, 1), jnp.where(number > 0, 0, -1), jnp.int32)
        return jnp.concatenate([own, first, picks], axis=1)
    return lax.map(one_block, jnp.arange(tile_index_sequence, dtype=jnp.int32))


def setup_inputs(seed: int = 0) -> dict:
    streams_of = jax.random.split(jax.random.key(seed), 6)
    queries = draw_queries(jax.random.fold_in(streams_of[5], 71), 0)
    keys = draw_keys(jax.random.fold_in(streams_of[5], 71), 0)
    values = draw_values(jax.random.fold_in(streams_of[5], 71), 0)
    selected = draw_selected(jax.random.fold_in(streams_of[5], 71), 0)
    norm_gain = jnp.clip(1.0 + 0.18 * jax.random.normal(streams_of[4], (QHEADS * HEAD_DIM,), jnp.float32), 0.099609375, 1.8984375).astype(jnp.bfloat16)
    return dict(queries=queries, keys=keys, values=values, selected=selected, norm_gain=norm_gain)


def reference(queries, keys, values, selected, norm_gain):
    tile_index_sequence = TOKENS // BLOCK
    group = QHEADS // KVHEADS
    scale = 1.0 / math.sqrt(HEAD_DIM)

    def by_head(array):
        return array.reshape(tile_index_sequence, BLOCK, KVHEADS, HEAD_DIM).transpose(2, 0, 1, 3)
    key_heads = by_head(keys)
    value_heads = by_head(values)
    head_iota = jnp.arange(KVHEADS, dtype=jnp.int32)[:, None]
    offsets = jnp.arange(BLOCK, dtype=jnp.int32)
    q_blocks = queries.reshape(tile_index_sequence, BLOCK, KVHEADS, group, HEAD_DIM)

    def attend(args):
        q_block, sel_row, number = args
        safe = jnp.clip(sel_row, 0, tile_index_sequence - 1).astype(jnp.int32)
        k_all = key_heads[head_iota, safe].reshape(KVHEADS, TOPK * BLOCK, HEAD_DIM).astype(jnp.float32)
        v_all = value_heads[head_iota, safe].reshape(KVHEADS, TOPK * BLOCK, HEAD_DIM).astype(jnp.float32)
        scores = jnp.einsum('tgrd,gkd->grtk', q_block.astype(jnp.float32), k_all) * scale
        key_pos = (sel_row[:, :, None] * BLOCK + offsets[None, None, :]).reshape(KVHEADS, TOPK * BLOCK)
        live = jnp.broadcast_to((sel_row >= 0)[:, :, None], (KVHEADS, TOPK, BLOCK)).reshape(KVHEADS, TOPK * BLOCK)
        query_pos = number * BLOCK + offsets
        mask = live[:, None, None, :] & (key_pos[:, None, None, :] <= query_pos[None, None, :, None])
        peak = lax.optimization_barrier(jnp.max(jnp.where(mask, scores, -1e+30), axis=-1, keepdims=True))
        weights = jnp.where(mask, jnp.exp(scores - peak), 0.0)
        total = lax.optimization_barrier(jnp.sum(weights, axis=-1))
        rounded = lax.optimization_barrier(weights.astype(jnp.bfloat16)).astype(jnp.float32)
        mixed = jnp.einsum('grtk,gkd->tgrd', rounded, v_all)
        return mixed / jnp.transpose(total, (2, 0, 1))[..., None]
    attended = lax.map(attend, (q_blocks, selected, jnp.arange(tile_index_sequence, dtype=jnp.int32)))
    attended = attended.reshape(TOKENS, QHEADS * HEAD_DIM)
    inverse = lax.rsqrt(lax.optimization_barrier(jnp.mean(attended * attended, axis=1)) + 1e-05)
    return (attended * inverse[:, None] * norm_gain.astype(jnp.float32)[None, :]).astype(jnp.bfloat16)
```

```python
import functools
import math

import jax
import jax.numpy as jnp
from jax import lax
from jax.experimental import pallas as pl
from jax.experimental.pallas import tpu as pltpu
from jax.sharding import PartitionSpec as P

NEG = -1e30


def attend_kernel(sel_ref, q_ref, kv_ref, att_ref, sq_ref, buf, sems, *, dims):
    per_dev, kv_local, top, block, head_dim, group = dims
    units = per_dev * kv_local
    width = 2 * head_dim
    exponent_scale = math.log2(math.e) / math.sqrt(head_dim)

    def fetch(unit, carry):
        col = pl.multiple_of(unit % kv_local * width, width)
        for entry in range(top):
            row = pl.multiple_of(jnp.maximum(sel_ref[unit * top + entry], 0) * block, block)
            pltpu.make_async_copy(
                kv_ref.at[pl.ds(row, block), pl.ds(col, width)],
                buf.at[unit, pl.ds(entry * block, block)],
                sems.at[unit],
            ).start()
        return carry

    lax.fori_loop(0, units, fetch, 0)

    lanes = 2 * block
    lane = lax.broadcasted_iota(jnp.int32, (1, lanes), 1)
    token = lax.broadcasted_iota(jnp.int32, (group * block, lanes), 0) % block
    column = lax.broadcasted_iota(jnp.int32, (group * block, lanes), 1)
    diagonal = jnp.where((column >= block) | (column <= token), 0.0, NEG)

    def attend(number, carry):
        rows = pl.ds(pl.multiple_of(number * block, block), block)
        squares = jnp.zeros((block, head_dim), jnp.float32)
        for g in range(kv_local):
            unit = number * kv_local + g
            pltpu.make_async_copy(
                kv_ref.at[pl.ds(0, top * block), pl.ds(0, width)], buf.at[unit], sems.at[unit]
            ).wait()
            heads = [
                slice((g * group + r) * head_dim, (g * group + r + 1) * head_dim)
                for r in range(group)
            ]
            q = jnp.concatenate([q_ref[rows, h] for h in heads], axis=0)
            keys = buf[unit, :, :head_dim]
            vals = buf[unit, :, head_dim:]
            scores = lax.dot_general(
                q, keys, (((1,), (1,)), ((), ())), preferred_element_type=jnp.float32
            )
            parts = []
            for pair in range(top // 2):
                low = jnp.where(sel_ref[unit * top + 2 * pair] >= 0, 0.0, NEG)
                high = jnp.where(sel_ref[unit * top + 2 * pair + 1] >= 0, 0.0, NEG)
                dead = jnp.where(lane < block, low, high)
                part = scores[:, pair * lanes : (pair + 1) * lanes] * exponent_scale + dead
                parts.append(part + diagonal if pair == 0 else part)
            peak = jnp.max(functools.reduce(jnp.maximum, parts), axis=1, keepdims=True)
            parts = [jnp.exp2(part - peak) for part in parts]
            total = jnp.sum(functools.reduce(jnp.add, parts), axis=1, keepdims=True)
            rounded = jnp.concatenate([part.astype(jnp.bfloat16) for part in parts], axis=1)
            mixed = jnp.dot(rounded, vals, preferred_element_type=jnp.float32) / total
            for r, h in enumerate(heads):
                piece = mixed[r * block : (r + 1) * block]
                att_ref[rows, h] = piece
                squares = squares + piece * piece
        sq_ref[rows, :] = squares
        return carry

    lax.fori_loop(0, per_dev, attend, 0)


def attend_blocks(selected, queries, pool, dims):
    per_dev, kv_local, top, block, head_dim, group = dims
    tokens = per_dev * block
    return pl.pallas_call(
        functools.partial(attend_kernel, dims=dims),
        out_shape=[
            jax.ShapeDtypeStruct(queries.shape, jnp.float32),
            jax.ShapeDtypeStruct((tokens, head_dim), jnp.float32),
        ],
        in_specs=[
            pl.BlockSpec(memory_space=pltpu.SMEM),
            pl.BlockSpec(memory_space=pltpu.VMEM),
            pl.BlockSpec(memory_space=pl.ANY),
        ],
        out_specs=[pl.BlockSpec(memory_space=pltpu.VMEM), pl.BlockSpec(memory_space=pltpu.VMEM)],
        scratch_shapes=[
            pltpu.VMEM((per_dev * kv_local, top * block, 2 * head_dim), jnp.bfloat16),
            pltpu.SemaphoreType.DMA((per_dev * kv_local,)),
        ],
        compiler_params=pltpu.CompilerParams(vmem_limit_bytes=40 * 1024 * 1024),
        name="attend",
    )(selected, queries, pool)


def per_device(queries, keys, values, selected, norm_gain):
    heads_axis = lax.axis_size("head")
    tok_dev = queries.shape[0]
    per_dev, kv_local, top = selected.shape
    block = tok_dev // per_dev
    head_dim = keys.shape[1] // kv_local
    group = queries.shape[1] // (kv_local * head_dim)
    dims = (per_dev, kv_local, top, block, head_dim, group)
    pieces = []
    for g in range(kv_local):
        cols = slice(g * head_dim, (g + 1) * head_dim)
        pieces += [keys[:, cols], values[:, cols]]
    pool = lax.all_gather(jnp.concatenate(pieces, axis=1), "seq", axis=0, tiled=True)
    attended, squares = attend_blocks(selected.reshape(-1), queries, pool, dims)
    local = jnp.sum(squares, axis=1)
    summed = local
    for shift in range(1, heads_axis):
        ring = [(i, (i + shift) % heads_axis) for i in range(heads_axis)]
        summed = summed + lax.ppermute(local, "head", ring)
    inverse = lax.rsqrt(summed / (queries.shape[1] * heads_axis) + 1e-05)
    normed = attended * inverse[:, None] * norm_gain.astype(jnp.float32)[None, :]
    return normed.astype(jnp.bfloat16)


def solution(mesh):
    return jax.shard_map(
        per_device,
        mesh=mesh,
        in_specs=(
            P("seq", "head"),
            P("seq", "head"),
            P("seq", "head"),
            P("seq", "head", None),
            P("head"),
        ),
        out_specs=P("seq", "head"),
        check_vma=False,
    )
```

```python
import functools
import math

import jax
import jax.numpy as jnp
from jax import lax
from jax.experimental import pallas as pl
from jax.experimental.pallas import tpu as pltpu
from jax.sharding import PartitionSpec as P

NEG = -1e30
KEY_SCALE = 8192.0
VALUE_SCALE = 4096.0


def attend_kernel(sel_ref, q_ref, chosen_ref, att_ref, sq_ref, *, dims):
    per_dev, kv_local, top, block, head_dim, group = dims
    exponent_scale = math.log2(math.e) / math.sqrt(head_dim) / KEY_SCALE
    lanes = 2 * block
    lane = lax.broadcasted_iota(jnp.int32, (1, lanes), 1)
    token = lax.broadcasted_iota(jnp.int32, (group * block, lanes), 0) % block
    column = lax.broadcasted_iota(jnp.int32, (group * block, lanes), 1)
    diagonal = jnp.where((column >= block) | (column <= token), 0.0, NEG)

    def attend(number, carry):
        rows = pl.ds(pl.multiple_of(number * block, block), block)
        squares = jnp.zeros((block, head_dim), jnp.float32)
        for g in range(kv_local):
            unit = number * kv_local + g
            heads = [
                slice((g * group + r) * head_dim, (g * group + r + 1) * head_dim)
                for r in range(group)
            ]
            q = jnp.concatenate([q_ref[rows, h] for h in heads], axis=0)
            keys = chosen_ref[unit, :, :head_dim]
            vals = chosen_ref[unit, :, head_dim:]
            scores = lax.dot_general(
                q, keys, (((1,), (1,)), ((), ())), preferred_element_type=jnp.float32
            )
            parts = []
            for pair in range(top // 2):
                low = jnp.where(sel_ref[unit * top + 2 * pair] >= 0, 0.0, NEG)
                high = jnp.where(sel_ref[unit * top + 2 * pair + 1] >= 0, 0.0, NEG)
                dead = jnp.where(lane < block, low, high)
                part = scores[:, pair * lanes : (pair + 1) * lanes] * exponent_scale + dead
                parts.append(part + diagonal if pair == 0 else part)
            peak = jnp.max(functools.reduce(jnp.maximum, parts), axis=1, keepdims=True)
            parts = [jnp.exp2(part - peak) for part in parts]
            total = jnp.sum(functools.reduce(jnp.add, parts), axis=1, keepdims=True)
            rounded = jnp.concatenate([part.astype(jnp.bfloat16) for part in parts], axis=1)
            mixed = jnp.dot(rounded, vals, preferred_element_type=jnp.float32)
            mixed = mixed / (total * VALUE_SCALE)
            for r, h in enumerate(heads):
                piece = mixed[r * block : (r + 1) * block]
                att_ref[rows, h] = piece
                squares = squares + piece * piece
        sq_ref[rows, :] = squares
        return carry

    lax.fori_loop(0, per_dev, attend, 0)


def attend_blocks(selected, queries, chosen, dims):
    per_dev, kv_local, top, block, head_dim, group = dims
    whole = pl.BlockSpec(memory_space=pltpu.VMEM)
    return pl.pallas_call(
        functools.partial(attend_kernel, dims=dims),
        out_shape=[
            jax.ShapeDtypeStruct(queries.shape, jnp.float32),
            jax.ShapeDtypeStruct((per_dev * block, head_dim), jnp.float32),
        ],
        in_specs=[pl.BlockSpec(memory_space=pltpu.SMEM), whole, whole],
        out_specs=[whole, whole],
        compiler_params=pltpu.CompilerParams(vmem_limit_bytes=40 * 1024 * 1024),
        name="attend",
    )(selected, queries, chosen)


def per_device(queries, keys, values, selected, norm_gain):
    heads_axis = lax.axis_size("head")
    tok_dev = queries.shape[0]
    per_dev, kv_local, top = selected.shape
    block = tok_dev // per_dev
    head_dim = keys.shape[1] // kv_local
    group = queries.shape[1] // (kv_local * head_dim)
    dims = (per_dev, kv_local, top, block, head_dim, group)
    codes = per_dev * kv_local

    def by_code(array, scale):
        rows = array.reshape(per_dev, block, kv_local, head_dim).transpose(0, 2, 1, 3)
        scaled = rows.reshape(codes, block, head_dim).astype(jnp.float32) * scale
        return scaled.astype(jnp.float16)

    stock = jnp.concatenate([by_code(keys, KEY_SCALE), by_code(values, VALUE_SCALE)], axis=2)
    pool = lax.all_gather(stock, "seq", axis=0, tiled=True)
    head_iota = jnp.arange(kv_local, dtype=jnp.int32)[None, :, None]
    index = (jnp.maximum(selected, 0) * kv_local + head_iota).reshape(-1)
    chosen = jnp.take(pool, index, axis=0, mode="clip").astype(jnp.bfloat16)
    chosen = chosen.reshape(codes, top * block, 2 * head_dim)
    flat = selected.reshape(-1)
    attended, squares = attend_blocks(flat, queries, chosen, dims)
    local = jnp.sum(squares, axis=1)
    copies = jnp.broadcast_to(local, (heads_axis, 1, tok_dev))
    everyone = lax.all_to_all(copies, "head", split_axis=0, concat_axis=0, tiled=True)
    summed = jnp.sum(everyone, axis=(0, 1))
    inverse = lax.rsqrt(summed / (queries.shape[1] * heads_axis) + 1e-05)
    normed = attended * inverse[:, None] * norm_gain.astype(jnp.float32)[None, :]
    return normed.astype(jnp.bfloat16)


def solution(mesh):
    return jax.shard_map(
        per_device,
        mesh=mesh,
        in_specs=(
            P("seq", "head"),
            P("seq", "head"),
            P("seq", "head"),
            P("seq", "head", None),
            P("head"),
        ),
        out_specs=P("seq", "head"),
        check_vma=False,
    )
```

```python
import functools
import math

import jax
import jax.numpy as jnp
from jax import lax
from jax.experimental import pallas as pl
from jax.experimental.pallas import tpu as pltpu
from jax.sharding import PartitionSpec as P

NEG = -1e30
KEY_SCALE = 8192.0
VALUE_SCALE = 4096.0


def attend_kernel(sel_ref, q_ref, *refs, dims):
    per_dev, kv_local, top, block, head_dim, group = dims
    tiles, (att_ref, sq_ref) = refs[:top], refs[top:]
    unit = pl.program_id(0)
    exponent_scale = math.log2(math.e) / math.sqrt(head_dim) / KEY_SCALE
    lanes = 2 * block
    lane = lax.broadcasted_iota(jnp.int32, (1, lanes), 1)
    token = lax.broadcasted_iota(jnp.int32, (group * block, lanes), 0) % block
    column = lax.broadcasted_iota(jnp.int32, (group * block, lanes), 1)
    diagonal = jnp.where((column >= block) | (column <= token), 0.0, NEG)
    heads = [slice(r * head_dim, (r + 1) * head_dim) for r in range(group)]
    q = jnp.concatenate([q_ref[:, h] for h in heads], axis=0)
    keys = jnp.concatenate([tile[0, :, :head_dim] for tile in tiles], axis=0)
    vals = jnp.concatenate([tile[0, :, head_dim:] for tile in tiles], axis=0)
    scores = lax.dot_general(q, keys, (((1,), (1,)), ((), ())), preferred_element_type=jnp.float32)
    parts = []
    for pair in range(top // 2):
        low = jnp.where(sel_ref[unit * top + 2 * pair] >= 0, 0.0, NEG)
        high = jnp.where(sel_ref[unit * top + 2 * pair + 1] >= 0, 0.0, NEG)
        dead = jnp.where(lane < block, low, high)
        part = scores[:, pair * lanes : (pair + 1) * lanes] * exponent_scale + dead
        parts.append(part + diagonal if pair == 0 else part)
    peak = jnp.max(functools.reduce(jnp.maximum, parts), axis=1, keepdims=True)
    parts = [jnp.exp2(part - peak) for part in parts]
    total = jnp.sum(functools.reduce(jnp.add, parts), axis=1, keepdims=True)
    rounded = jnp.concatenate([part.astype(jnp.bfloat16) for part in parts], axis=1)
    mixed = jnp.dot(rounded, vals, preferred_element_type=jnp.float32)
    mixed = mixed / (total * VALUE_SCALE)
    squares = jnp.zeros((block, head_dim), jnp.float32)
    for r, h in enumerate(heads):
        piece = mixed[r * block : (r + 1) * block]
        att_ref[:, h] = piece
        squares = squares + piece * piece

    @pl.when(unit % kv_local == 0)
    def _():
        sq_ref[...] = squares

    @pl.when(unit % kv_local != 0)
    def _():
        sq_ref[...] = sq_ref[...] + squares


def attend_blocks(selected, queries, pool, dims):
    per_dev, kv_local, top, block, head_dim, group = dims

    def tile_index(entry, unit, sel):
        return (jnp.maximum(sel[unit * top + entry], 0) * kv_local + unit % kv_local, 0, 0)

    heads = pl.BlockSpec(
        (block, group * head_dim), lambda unit, sel: (unit // kv_local, unit % kv_local)
    )
    tiles = [
        pl.BlockSpec((1, block, 2 * head_dim), functools.partial(tile_index, entry))
        for entry in range(top)
    ]
    return pl.pallas_call(
        functools.partial(attend_kernel, dims=dims),
        grid_spec=pltpu.PrefetchScalarGridSpec(
            num_scalar_prefetch=1,
            grid=(per_dev * kv_local,),
            in_specs=[heads] + tiles,
            out_specs=[
                heads,
                pl.BlockSpec((block, head_dim), lambda unit, sel: (unit // kv_local, 0)),
            ],
        ),
        out_shape=[
            jax.ShapeDtypeStruct(queries.shape, jnp.float32),
            jax.ShapeDtypeStruct((per_dev * block, head_dim), jnp.float32),
        ],
        compiler_params=pltpu.CompilerParams(
            vmem_limit_bytes=40 * 1024 * 1024,
            allow_input_fusion=[False, False] + [True] * top,
        ),
        name="attend",
    )(selected, queries, *([pool.astype(jnp.bfloat16)] * top))


def per_device(queries, keys, values, selected, norm_gain):
    heads_axis = lax.axis_size("head")
    tok_dev = queries.shape[0]
    per_dev, kv_local, top = selected.shape
    block = tok_dev // per_dev
    head_dim = keys.shape[1] // kv_local
    group = queries.shape[1] // (kv_local * head_dim)
    dims = (per_dev, kv_local, top, block, head_dim, group)
    codes = per_dev * kv_local

    def by_code(array, scale):
        rows = array.reshape(per_dev, block, kv_local, head_dim).transpose(0, 2, 1, 3)
        scaled = rows.reshape(codes, block, head_dim).astype(jnp.float32) * scale
        return scaled.astype(jnp.float16)

    stock = jnp.concatenate([by_code(keys, KEY_SCALE), by_code(values, VALUE_SCALE)], axis=2)
    pool = lax.all_gather(stock, "seq", axis=0, tiled=True)
    attended, squares = attend_blocks(selected.reshape(-1), queries, pool, dims)
    local = jnp.sum(squares, axis=1)
    copies = jnp.broadcast_to(local, (heads_axis, 1, tok_dev))
    everyone = lax.all_to_all(copies, "head", split_axis=0, concat_axis=0, tiled=True)
    summed = jnp.sum(everyone, axis=(0, 1))
    inverse = lax.rsqrt(summed / (queries.shape[1] * heads_axis) + 1e-05)
    normed = attended * inverse[:, None] * norm_gain.astype(jnp.float32)[None, :]
    return normed.astype(jnp.bfloat16)


def solution(mesh):
    return jax.shard_map(
        per_device,
        mesh=mesh,
        in_specs=(
            P("seq", "head"),
            P("seq", "head"),
            P("seq", "head"),
            P("seq", "head", None),
            P("head"),
        ),
        out_specs=P("seq", "head"),
        check_vma=False,
    )
```

```python
import functools
import math

import jax
import jax.numpy as jnp
from jax import lax
from jax.experimental import pallas as pl
from jax.experimental.pallas import tpu as pltpu
from jax.sharding import PartitionSpec as P

NEG = -1e30
KEY_SCALE = 8192.0
VALUE_SCALE = 4096.0


def attend_kernel(sel_ref, q_ref, *refs, dims):
    per_dev, kv_local, top, block, head_dim, group = dims
    att_ref, sq_ref = refs[per_dev * kv_local * top :]
    exponent_scale = math.log2(math.e) / math.sqrt(head_dim) / KEY_SCALE
    lanes = 2 * block
    lane = lax.broadcasted_iota(jnp.int32, (1, lanes), 1)
    token = lax.broadcasted_iota(jnp.int32, (group * block, lanes), 0) % block
    column = lax.broadcasted_iota(jnp.int32, (group * block, lanes), 1)
    diagonal = jnp.where((column >= block) | (column <= token), 0.0, NEG)
    every = []
    for number in range(per_dev):
        rows = slice(number * block, (number + 1) * block)
        squares = jnp.zeros((block, head_dim), jnp.float32)
        for g in range(kv_local):
            unit = number * kv_local + g
            tiles = refs[unit * top : (unit + 1) * top]
            heads = [
                slice((g * group + r) * head_dim, (g * group + r + 1) * head_dim) for r in range(group)
            ]
            q = jnp.concatenate([q_ref[rows, h] for h in heads], axis=0)
            keys = jnp.concatenate([tile[0, :, :head_dim] for tile in tiles], axis=0)
            vals = jnp.concatenate([tile[0, :, head_dim:] for tile in tiles], axis=0)
            scores = lax.dot_general(
                q, keys, (((1,), (1,)), ((), ())), preferred_element_type=jnp.float32
            )
            parts = []
            for pair in range(top // 2):
                low = jnp.where(sel_ref[unit * top + 2 * pair] >= 0, 0.0, NEG)
                high = jnp.where(sel_ref[unit * top + 2 * pair + 1] >= 0, 0.0, NEG)
                dead = jnp.where(lane < block, low, high)
                part = scores[:, pair * lanes : (pair + 1) * lanes] * exponent_scale + dead
                parts.append(part + diagonal if pair == 0 else part)
            peak = jnp.max(functools.reduce(jnp.maximum, parts), axis=1, keepdims=True)
            parts = [jnp.exp2(part - peak) for part in parts]
            total = jnp.sum(functools.reduce(jnp.add, parts), axis=1, keepdims=True)
            rounded = jnp.concatenate([part.astype(jnp.bfloat16) for part in parts], axis=1)
            mixed = jnp.dot(rounded, vals, preferred_element_type=jnp.float32)
            mixed = mixed / (total * VALUE_SCALE)
            for r, h in enumerate(heads):
                piece = mixed[r * block : (r + 1) * block]
                att_ref[rows, h] = piece
                squares = squares + piece * piece
        every.append(squares)
    ones = jnp.ones((8, head_dim), jnp.float32)
    sums = lax.dot_general(
        ones,
        jnp.concatenate(every, axis=0),
        (((1,), (1,)), ((), ())),
        precision=lax.Precision.HIGHEST,
        preferred_element_type=jnp.float32,
    )
    for copy in range(sq_ref.shape[0]):
        sq_ref[copy] = sums[:1]


def attend_blocks(selected, queries, pool, dims, copies):
    per_dev, kv_local, top, block, head_dim, group = dims
    windows = per_dev * kv_local * top

    def tile_index(place, step, sel):
        return (jnp.maximum(sel[place], 0) * kv_local + place // top % kv_local, 0, 0)

    rows = pl.BlockSpec(queries.shape, lambda step, sel: (0, 0))
    tiles = [
        pl.BlockSpec((1, block, 2 * head_dim), functools.partial(tile_index, place))
        for place in range(windows)
    ]
    sums = (copies, 1, per_dev * block)
    return pl.pallas_call(
        functools.partial(attend_kernel, dims=dims),
        grid_spec=pltpu.PrefetchScalarGridSpec(
            num_scalar_prefetch=1,
            grid=(1,),
            in_specs=[rows] + tiles,
            out_specs=[rows, pl.BlockSpec(sums, lambda step, sel: (0, 0, 0))],
        ),
        out_shape=[
            jax.ShapeDtypeStruct(queries.shape, jnp.float32),
            jax.ShapeDtypeStruct(sums, jnp.float32),
        ],
        compiler_params=pltpu.CompilerParams(
            vmem_limit_bytes=40 * 1024 * 1024,
            allow_input_fusion=[False, False] + [True] * windows,
        ),
        name="attend",
    )(selected, queries, *([pool.astype(jnp.bfloat16)] * windows))


def per_device(queries, keys, values, selected, norm_gain):
    heads_axis = lax.axis_size("head")
    tok_dev = queries.shape[0]
    per_dev, kv_local, top = selected.shape
    block = tok_dev // per_dev
    head_dim = keys.shape[1] // kv_local
    group = queries.shape[1] // (kv_local * head_dim)
    dims = (per_dev, kv_local, top, block, head_dim, group)
    columns = jnp.arange(2 * kv_local * head_dim)[None, :]
    scales = jnp.where(columns < kv_local * head_dim, KEY_SCALE, VALUE_SCALE)
    rows = jnp.concatenate([keys, values], axis=1).astype(jnp.float32) * scales
    rows = lax.optimization_barrier(rows.astype(jnp.float16))
    tiles = [
        rows[:, c * head_dim : (c + 1) * head_dim].reshape(per_dev, block, head_dim)
        for c in range(2 * kv_local)
    ]
    pairs = [jnp.concatenate([tiles[g], tiles[kv_local + g]], axis=2) for g in range(kv_local)]
    stock = jnp.stack(pairs, axis=1).reshape(per_dev * kv_local, block, 2 * head_dim)
    pool = lax.all_gather(stock, "seq", axis=0, tiled=True)
    attended, copies = attend_blocks(selected.reshape(-1), queries, pool, dims, heads_axis)
    everyone = lax.all_to_all(copies, "head", split_axis=0, concat_axis=0, tiled=True)
    summed = jnp.sum(everyone, axis=(0, 1))
    inverse = lax.rsqrt(summed / (queries.shape[1] * heads_axis) + 1e-05)
    normed = attended * inverse[:, None] * norm_gain.astype(jnp.float32)[None, :]
    return normed.astype(jnp.bfloat16)


def solution(mesh):
    return jax.shard_map(
        per_device,
        mesh=mesh,
        in_specs=(
            P("seq", "head"),
            P("seq", "head"),
            P("seq", "head"),
            P("seq", "head", None),
            P("head"),
        ),
        out_specs=P("seq", "head"),
        check_vma=False,
    )
```

```python
import functools
import math

import jax
import jax.numpy as jnp
from jax import lax
from jax.experimental import pallas as pl
from jax.experimental.pallas import tpu as pltpu
from jax.sharding import PartitionSpec as P

NEG = -1e30
KEY_SCALE = 8192.0
VALUE_SCALE = 4096.0


def attend_kernel(sel_ref, q_ref, *refs, dims):
    per_dev, kv_local, top, block, head_dim, group = dims
    att_ref, sq_ref = refs[per_dev * kv_local * top :]
    exponent_scale = math.log2(math.e) / math.sqrt(head_dim) / KEY_SCALE
    lanes = 2 * block
    lane = lax.broadcasted_iota(jnp.int32, (1, lanes), 1)
    token = lax.broadcasted_iota(jnp.int32, (group * block, lanes), 0) % block
    column = lax.broadcasted_iota(jnp.int32, (group * block, lanes), 1)
    diagonal = jnp.where((column >= block) | (column <= token), 0.0, NEG)
    every = []
    for number in range(per_dev):
        rows = slice(number * block, (number + 1) * block)
        squares = jnp.zeros((block, head_dim), jnp.float32)
        for g in range(kv_local):
            unit = number * kv_local + g
            tiles = refs[unit * top : (unit + 1) * top]
            heads = [
                slice((g * group + r) * head_dim, (g * group + r + 1) * head_dim) for r in range(group)
            ]
            q = jnp.concatenate([q_ref[rows, h] for h in heads], axis=0)
            keys = jnp.concatenate([tile[0, :, :head_dim] for tile in tiles], axis=0)
            vals = jnp.concatenate([tile[0, :, head_dim:] for tile in tiles], axis=0)
            scores = lax.dot_general(
                q, keys, (((1,), (1,)), ((), ())), preferred_element_type=jnp.float32
            )
            parts = []
            for pair in range(top // 2):
                low = jnp.where(sel_ref[unit * top + 2 * pair] >= 0, 0.0, NEG)
                high = jnp.where(sel_ref[unit * top + 2 * pair + 1] >= 0, 0.0, NEG)
                dead = jnp.where(lane < block, low, high)
                part = scores[:, pair * lanes : (pair + 1) * lanes] * exponent_scale + dead
                parts.append(part + diagonal if pair == 0 else part)
            peak = jnp.max(functools.reduce(jnp.maximum, parts), axis=1, keepdims=True)
            parts = [jnp.exp2(part - peak) for part in parts]
            total = jnp.sum(functools.reduce(jnp.add, parts), axis=1, keepdims=True)
            rounded = jnp.concatenate([part.astype(jnp.bfloat16) for part in parts], axis=1)
            mixed = jnp.dot(rounded, vals, preferred_element_type=jnp.float32)
            mixed = mixed / (total * VALUE_SCALE)
            for r, h in enumerate(heads):
                piece = mixed[r * block : (r + 1) * block]
                att_ref[rows, h] = piece
                squares = squares + piece * piece
        every.append(squares)
    ones = jnp.ones((8, head_dim), jnp.float32)
    sums = lax.dot_general(
        ones,
        jnp.concatenate(every, axis=0),
        (((1,), (1,)), ((), ())),
        precision=lax.Precision.HIGHEST,
        preferred_element_type=jnp.float32,
    )
    for copy in range(sq_ref.shape[0]):
        sq_ref[copy] = sums[:1]


def attend_blocks(selected, queries, pool, dims, copies):
    per_dev, kv_local, top, block, head_dim, group = dims
    windows = per_dev * kv_local * top

    def tile_index(place, step, sel):
        block_index = jnp.where(sel[place] >= 0, sel[place], place)
        return (block_index * kv_local + place // top % kv_local, 0, 0)

    rows = pl.BlockSpec(queries.shape, lambda step, sel: (0, 0))
    tiles = [
        pl.BlockSpec((1, block, 2 * head_dim), functools.partial(tile_index, place))
        for place in range(windows)
    ]
    sums = (copies, 1, per_dev * block)
    return pl.pallas_call(
        functools.partial(attend_kernel, dims=dims),
        grid_spec=pltpu.PrefetchScalarGridSpec(
            num_scalar_prefetch=1,
            grid=(1,),
            in_specs=[rows] + tiles,
            out_specs=[rows, pl.BlockSpec(sums, lambda step, sel: (0, 0, 0))],
        ),
        out_shape=[
            jax.ShapeDtypeStruct(queries.shape, jnp.float32),
            jax.ShapeDtypeStruct(sums, jnp.float32),
        ],
        compiler_params=pltpu.CompilerParams(
            vmem_limit_bytes=40 * 1024 * 1024,
            allow_input_fusion=[False, False] + [True] * windows,
        ),
        name="attend",
    )(selected, queries, *([pool.astype(jnp.bfloat16)] * windows))


def per_device(queries, keys, values, selected, norm_gain):
    heads_axis = lax.axis_size("head")
    tok_dev = queries.shape[0]
    per_dev, kv_local, top = selected.shape
    block = tok_dev // per_dev
    head_dim = keys.shape[1] // kv_local
    group = queries.shape[1] // (kv_local * head_dim)
    dims = (per_dev, kv_local, top, block, head_dim, group)
    columns = jnp.arange(2 * kv_local * head_dim)[None, :]
    scales = jnp.where(columns < kv_local * head_dim, KEY_SCALE, VALUE_SCALE)
    rows = jnp.concatenate([keys, values], axis=1).astype(jnp.float32) * scales
    rows = lax.optimization_barrier(rows.astype(jnp.float16))
    tiles = [
        rows[:, c * head_dim : (c + 1) * head_dim].reshape(per_dev, block, head_dim)
        for c in range(2 * kv_local)
    ]
    pairs = [jnp.concatenate([tiles[g], tiles[kv_local + g]], axis=2) for g in range(kv_local)]
    stock = jnp.stack(pairs, axis=1).reshape(per_dev * kv_local, block, 2 * head_dim)
    pool = lax.all_gather(stock, "seq", axis=0, tiled=True)
    attended, copies = attend_blocks(selected.reshape(-1), queries, pool, dims, heads_axis)
    everyone = lax.all_to_all(copies, "head", split_axis=0, concat_axis=0, tiled=True)
    summed = jnp.sum(everyone, axis=(0, 1))
    inverse = lax.rsqrt(summed / (queries.shape[1] * heads_axis) + 1e-05)
    normed = attended * inverse[:, None] * norm_gain.astype(jnp.float32)[None, :]
    return normed.astype(jnp.bfloat16)


def solution(mesh):
    return jax.shard_map(
        per_device,
        mesh=mesh,
        in_specs=(
            P("seq", "head"),
            P("seq", "head"),
            P("seq", "head"),
            P("seq", "head", None),
            P("head"),
        ),
        out_specs=P("seq", "head"),
        check_vma=False,
    )
```

```python
import functools
import math

import jax
import jax.numpy as jnp
from jax import lax
from jax.experimental import pallas as pl
from jax.experimental.pallas import tpu as pltpu
from jax.sharding import PartitionSpec as P

NEG = -1e30
KEY_SCALE = 8192.0
VALUE_SCALE = 4096.0


def attend_kernel(sel_ref, q_ref, *refs, dims):
    per_dev, kv_local, top, block, head_dim, group = dims
    att_ref, sq_ref = refs[per_dev * kv_local * (top - 1) + kv_local :]
    shared = per_dev * kv_local * (top - 1)
    exponent_scale = math.log2(math.e) / math.sqrt(head_dim) / KEY_SCALE
    lanes = 2 * block
    lane = lax.broadcasted_iota(jnp.int32, (1, lanes), 1)
    token = lax.broadcasted_iota(jnp.int32, (group * block, lanes), 0) % block
    column = lax.broadcasted_iota(jnp.int32, (group * block, lanes), 1)
    diagonal = jnp.where((column >= block) | (column <= token), 0.0, NEG)
    every = []
    for number in range(per_dev):
        rows = slice(number * block, (number + 1) * block)
        squares = jnp.zeros((block, head_dim), jnp.float32)
        for g in range(kv_local):
            unit = number * kv_local + g
            own = unit * (top - 1)
            tiles = (refs[own], refs[shared + g]) + refs[own + 1 : own + top - 1]
            heads = [
                slice((g * group + r) * head_dim, (g * group + r + 1) * head_dim) for r in range(group)
            ]
            q = jnp.concatenate([q_ref[rows, h] for h in heads], axis=0)
            keys = jnp.concatenate([tile[0, :, :head_dim] for tile in tiles], axis=0)
            vals = jnp.concatenate([tile[0, :, head_dim:] for tile in tiles], axis=0)
            scores = lax.dot_general(
                q, keys, (((1,), (1,)), ((), ())), preferred_element_type=jnp.float32
            )
            parts = []
            for pair in range(top // 2):
                low = jnp.where(sel_ref[unit * top + 2 * pair] >= 0, 0.0, NEG)
                high = jnp.where(sel_ref[unit * top + 2 * pair + 1] >= 0, 0.0, NEG)
                dead = jnp.where(lane < block, low, high)
                part = scores[:, pair * lanes : (pair + 1) * lanes] * exponent_scale + dead
                parts.append(part + diagonal if pair == 0 else part)
            peak = jnp.max(functools.reduce(jnp.maximum, parts), axis=1, keepdims=True)
            parts = [jnp.exp2(part - peak) for part in parts]
            total = jnp.sum(functools.reduce(jnp.add, parts), axis=1, keepdims=True)
            rounded = jnp.concatenate([part.astype(jnp.bfloat16) for part in parts], axis=1)
            mixed = jnp.dot(rounded, vals, preferred_element_type=jnp.float32)
            mixed = mixed / (total * VALUE_SCALE)
            for r, h in enumerate(heads):
                piece = mixed[r * block : (r + 1) * block]
                att_ref[rows, h] = piece
                squares = squares + piece * piece
        every.append(squares)
    ones = jnp.ones((8, head_dim), jnp.float32)
    sums = lax.dot_general(
        ones,
        jnp.concatenate(every, axis=0),
        (((1,), (1,)), ((), ())),
        precision=lax.Precision.HIGHEST,
        preferred_element_type=jnp.float32,
    )
    for copy in range(sq_ref.shape[0]):
        sq_ref[copy] = sums[:1]


def attend_blocks(selected, queries, pool, dims, copies):
    per_dev, kv_local, top, block, head_dim, group = dims

    def tile_index(place, step, sel):
        block_index = jnp.where(sel[place] >= 0, sel[place], place)
        return (block_index * kv_local + place // top % kv_local, 0, 0)

    def first_index(g, step, sel):
        return (g, 0, 0)

    rows = pl.BlockSpec(queries.shape, lambda step, sel: (0, 0))
    shape = (1, block, 2 * head_dim)
    tiles = [
        pl.BlockSpec(shape, functools.partial(tile_index, place))
        for place in range(per_dev * kv_local * top)
        if place % top != 1
    ] + [pl.BlockSpec(shape, functools.partial(first_index, g)) for g in range(kv_local)]
    windows = len(tiles)
    sums = (copies, 1, per_dev * block)
    return pl.pallas_call(
        functools.partial(attend_kernel, dims=dims),
        grid_spec=pltpu.PrefetchScalarGridSpec(
            num_scalar_prefetch=1,
            grid=(1,),
            in_specs=[rows] + tiles,
            out_specs=[rows, pl.BlockSpec(sums, lambda step, sel: (0, 0, 0))],
        ),
        out_shape=[
            jax.ShapeDtypeStruct(queries.shape, jnp.float32),
            jax.ShapeDtypeStruct(sums, jnp.float32),
        ],
        compiler_params=pltpu.CompilerParams(
            vmem_limit_bytes=40 * 1024 * 1024,
            allow_input_fusion=[False, False] + [True] * windows,
        ),
        name="attend",
    )(selected, queries, *([pool.astype(jnp.bfloat16)] * windows))


def per_device(queries, keys, values, selected, norm_gain):
    heads_axis = lax.axis_size("head")
    tok_dev = queries.shape[0]
    per_dev, kv_local, top = selected.shape
    block = tok_dev // per_dev
    head_dim = keys.shape[1] // kv_local
    group = queries.shape[1] // (kv_local * head_dim)
    dims = (per_dev, kv_local, top, block, head_dim, group)
    columns = jnp.arange(2 * kv_local * head_dim)[None, :]
    scales = jnp.where(columns < kv_local * head_dim, KEY_SCALE, VALUE_SCALE)
    rows = jnp.concatenate([keys, values], axis=1).astype(jnp.float32) * scales
    rows = lax.optimization_barrier(rows.astype(jnp.float16))
    tiles = [
        rows[:, c * head_dim : (c + 1) * head_dim].reshape(per_dev, block, head_dim)
        for c in range(2 * kv_local)
    ]
    pairs = [jnp.concatenate([tiles[g], tiles[kv_local + g]], axis=2) for g in range(kv_local)]
    stock = jnp.stack(pairs, axis=1).reshape(per_dev * kv_local, block, 2 * head_dim)
    pool = lax.all_gather(stock, "seq", axis=0, tiled=True)
    attended, copies = attend_blocks(selected.reshape(-1), queries, pool, dims, heads_axis)
    everyone = lax.all_to_all(copies, "head", split_axis=0, concat_axis=0, tiled=True)
    summed = jnp.sum(everyone, axis=(0, 1))
    inverse = lax.rsqrt(summed / (queries.shape[1] * heads_axis) + 1e-05)
    normed = attended * inverse[:, None] * norm_gain.astype(jnp.float32)[None, :]
    return normed.astype(jnp.bfloat16)


def solution(mesh):
    return jax.shard_map(
        per_device,
        mesh=mesh,
        in_specs=(
            P("seq", "head"),
            P("seq", "head"),
            P("seq", "head"),
            P("seq", "head", None),
            P("head"),
        ),
        out_specs=P("seq", "head"),
        check_vma=False,
    )
```
